32 devices in a mesh: batch: 4 (over x, core), vocab: 8 (over z, y).
Axes of the slice: x: 2, y: 2, z: 4, core: 2. Of those that a mesh axis runs over, the one named last changes fastest.
Arguments:
- hidden_rows: bfloat16 [4096, 4096], P(('batch', 'vocab')), parts along dimension 0
- head_weight: bfloat16 [4096, 10240], P(None, 'vocab'), may hold values from -0.09375 to 0.09375
- draft_ids: int32 [64, 64], P('batch'), parts along dimension 0, may hold values from 0 to 10239
- parents: int32 [64, 64], P('batch'), parts along dimension 0, may hold values from 0 to 62, as said below
Outputs:
- log_total: float32 [64, 64], P('batch'), parts along dimension 0
- draft_logp: float32 [64, 64], P('batch'), parts along dimension 0
- path_sum: float32 [64, 64], P('batch'), parts along dimension 0
The draws below stay inside these ranges and needn't reach their ends.
There are 4 independent parts, one for each index of `batch`. The reference program is written for one: setup_inputs(seed, part) draws one part's arguments, and reference() takes and returns one part's arrays. A program takes and returns all parts, laid end to end along the dimension named above; an argument that names none is the same for every part. Nothing has to cross between parts.
Inputs may be any that keep to these rules, and one draw needn't show every extreme that they name: parents[s, 0] = 0 for every sequence, and parents[s, n] lies in 0 to n - 1 for n > 0, so that every node's ancestors lead to node 0.
All inputs are finite; a program needn't handle non-finite values.
Results may differ from the reference program's by a relative error of at most 0.0003.
Values may be sent and summed in bfloat16 or wider, within the bound.
A program may use at most 128 MiB of HBM per device.

```python
import jax
import jax.numpy as jnp
from jax import lax

D = 4096
NODES = 64
SEQS = 16
VOCAB = 10240
ROWS = 1024


def draw_hidden_rows(key, part):
    base_key = jax.random.fold_in(key, 11)
    return (3.0 * jax.random.normal(base_key, (ROWS, D), jnp.float32)).astype(jnp.bfloat16)


def draw_parents(key, part):
    limits = jnp.maximum(jnp.arange(NODES, dtype=jnp.int32), 1)
    drawn = jax.random.randint(jax.random.fold_in(key, 21), (SEQS, NODES), 0, limits, dtype=jnp.int32)
    return drawn.at[0, NODES - 1].set(NODES - 2)


def place_ends(values, key, low, largest):
    longest = values.shape.index(max(values.shape))
    spots = []
    for shift in (0, 1):
        where = [jax.random.randint(jax.random.fold_in(key, axis), (), 0, length) for axis, length in enumerate(values.shape)]
        where[longest] = (where[longest] + shift) % values.shape[longest]
        spots.append(tuple(where))
    return values.at[spots[0]].set(low).at[spots[1]].set(largest)


def block_levels(key, shape, shards, least, high):
    gain, own = 1.0, jax.random.fold_in(key, 6)
    for dim, shards_of in shards:
        heights = jnp.exp(jax.random.uniform(jax.random.fold_in(own, dim), (shards_of,), jnp.float32, least / len(shards), high / len(shards)))
        gain = gain * jnp.repeat(heights, shape[dim] // shards_of).reshape([-1 if axis == dim else 1 for axis in range(len(shape))])
    return gain


def scatter_about(own_key, shape, spread, limit, pieces=(), kind=jnp.bfloat16):
    array = spread * jax.random.normal(own_key, shape, jnp.float32)
    if pieces:
        array = array * block_levels(own_key, shape, pieces, -0.22, 0.18)
    return jnp.clip(array, -limit, limit).astype(kind)


def setup_inputs(seed: int = 0, part: int = 0) -> dict:
    seeds = jax.random.split(jax.random.key(seed), 5)
    own_keys = jax.random.split(jax.random.fold_in(seeds[4], part), 5)
    hidden_rows = draw_hidden_rows(jax.random.fold_in(jax.random.fold_in(seeds[4], part), 71), part)
    head_weight = scatter_about(seeds[1], (D, VOCAB), D ** -0.5, 0.09375, ((1, 8),))
    draft_ids = place_ends(jax.random.randint(own_keys[2], (SEQS, NODES), 0, VOCAB), jax.random.fold_in(own_keys[2], 1), 0, VOCAB - 1).astype(jnp.int32)
    parents = draw_parents(jax.random.fold_in(jax.random.fold_in(seeds[4], part), 71), part)
    return dict(hidden_rows=hidden_rows, head_weight=head_weight, draft_ids=draft_ids, parents=parents)


def reference(hidden_rows, head_weight, draft_ids, parents):
    seq_count, node_count = draft_ids.shape
    hidden_seqs = hidden_rows.reshape(seq_count, node_count, hidden_rows.shape[1])

    def one_sequence(inputs):
        rows_here, drafts_here, parents_here = inputs
        logits = jnp.dot(rows_here, head_weight, preferred_element_type=jnp.float32)
        row_top = jnp.max(logits, axis=1)
        log_total = row_top + jnp.log(jnp.sum(jnp.exp(logits - row_top[:, None]), axis=1))
        target = logits[parents_here, drafts_here]
        node_ids = jnp.arange(node_count, dtype=jnp.int32)
        draft_logp = jnp.where(node_ids > 0, target - log_total[parents_here], jnp.zeros_like(target))
        return log_total, draft_logp

    log_total, draft_logp = lax.map(one_sequence, (hidden_seqs, draft_ids, parents))

    def extend(node, path_sum):
        parent_col = lax.dynamic_index_in_dim(parents, node, 1, keepdims=True).astype(jnp.int32)
        above = jnp.take_along_axis(path_sum, parent_col, axis=1)[:, 0]
        own = lax.dynamic_index_in_dim(draft_logp, node, 1, keepdims=False)
        return path_sum.at[:, node].set(own + above)

    path_sum = lax.fori_loop(1, node_count, extend, jnp.zeros_like(draft_logp))
    return (log_total, draft_logp, path_sum)
```

```python
import functools

import jax
import jax.numpy as jnp
from jax import lax
from jax.experimental import pallas as pl
from jax.experimental.pallas import tpu as pltpu
from jax.sharding import PartitionSpec as P

MESH = pl.DeviceIdType.MESH
LANES = 128
TILE = 256
SUB = 4
CHUNKS = 4


def general(hidden_rows, head_weight, draft_ids, parents):
    shard_width = head_weight.shape[1]
    offset = lax.axis_index("vocab") * shard_width
    gathered = lax.all_gather(hidden_rows, "vocab", axis=0, tiled=True)
    logits = jnp.dot(gathered, head_weight, preferred_element_type=jnp.float32)
    seq_count, node_count = draft_ids.shape
    node_ids = jnp.arange(node_count, dtype=jnp.int32)
    local_max = jnp.max(logits, axis=1)
    parent_rows = (jnp.arange(seq_count, dtype=jnp.int32)[:, None] * node_count + parents).reshape(
        -1
    )
    columns = draft_ids.reshape(-1) - offset
    inside = (columns >= 0) & (columns < shard_width)
    picked = jnp.take(
        logits.reshape(-1), parent_rows * shard_width + jnp.clip(columns, 0, shard_width - 1)
    )
    local_target = jnp.where(inside, picked, jnp.zeros_like(picked))
    row_top = lax.pmax(local_max, "vocab")
    local_sum = jnp.sum(jnp.exp(logits - row_top[:, None]), axis=1)
    row_total, target = lax.psum((local_sum, local_target), "vocab")
    log_total = (row_top + jnp.log(row_total)).reshape(seq_count, node_count)
    target = target.reshape(seq_count, node_count)
    choose = (parents[:, :, None] == node_ids[None, None, :]).astype(jnp.float32)
    log_parent = jnp.einsum("snr,sr->sn", choose, log_total, precision=lax.Precision.HIGHEST)
    draft_logp = jnp.where(node_ids[None, :] > 0, target - log_parent, jnp.zeros_like(target))
    path_sum = draft_logp
    jump_table = choose
    for jump_round in range((node_count - 1).bit_length()):
        path_sum = path_sum + jnp.einsum(
            "snr,sr->sn", jump_table, path_sum, precision=lax.Precision.HIGHEST
        )
        jump_table = jnp.einsum(
            "snr,srq->snq", jump_table, jump_table, precision=lax.Precision.HIGHEST
        )
    return (log_total, draft_logp, path_sum)


def plan(tiles):
    steps = {}
    for t in range(tiles):
        steps.setdefault(1 + t, []).append((0, t))
    for t in range(tiles):
        steps.setdefault(8 + t // 2, []).append((1, t))
        steps.setdefault(16 + t // 2, []).append((2, t))
    for j in range(tiles):
        ready = SUB * j + SUB + 1
        for o, come in ((0, 6), (1, 10), (2, 18)):
            steps.setdefault(max(ready, come), []).append((o, tiles + j))
    return steps


def table(index, values):
    out = jnp.int32(values[-1])
    for k in range(len(values) - 2, -1, -1):
        if values[k] != values[k + 1]:
            out = jnp.where(index <= k, jnp.int32(values[k]), out)
    return out


def split3(x):
    hi = x.astype(jnp.bfloat16)
    rest = x - hi.astype(jnp.float32)
    mid = rest.astype(jnp.bfloat16)
    lo = (rest - mid.astype(jnp.float32)).astype(jnp.bfloat16)
    return hi, mid, lo


def kernel(n, nodes, h_ref, w_ref, draft_ref, par_ref, lt_ref, dl_ref, ps_ref,
           rows, wv, lg, st, pick, anc, jump,
           up_s, dn_s, r_r, y_s, y_r, x_s, x_r, d_s, d_r, st_s, st_r, loc_w, loc_r):
    b, v = lax.axis_index("batch"), lax.axis_index("vocab")
    x, z, y = b // 2, v // 2, v % 2
    peers = 2 * n
    yp = v + 1 - 2 * y
    xb = b + 2 - 4 * x
    cb = b + 1 - 2 * (b % 2)
    cxb = cb + 2 - 4 * x
    count, depth = h_ref.shape
    width = w_ref.shape[1]
    tiles = width // TILE
    quarter = depth // 4
    piece = quarter // SUB
    part = count // CHUNKS
    total = tiles * SUB
    pairs = par_ref.shape[0]

    barrier = pltpu.get_barrier_semaphore()
    for k in range(1, peers):
        pl.semaphore_signal(barrier, inc=1, device_id=(b, lax.rem(v + k, peers)), device_id_type=MESH)
    pl.semaphore_signal(barrier, inc=1, device_id=(cb, v), device_id_type=MESH)
    pl.semaphore_signal(barrier, inc=1, device_id=(xb, v), device_id_type=MESH)

    def own_w(t):
        return pltpu.make_async_copy(w_ref.at[:, pl.ds(t * TILE, TILE)], wv.at[t], loc_w.at[t])

    own_rows = pltpu.make_async_copy(h_ref, rows.at[z], loc_r)
    own_rows.start()
    for t in range(tiles):
        own_w(t).start()
    pl.semaphore_wait(barrier, peers + 1)

    def hop(src, k, there, send, own):
        here = h_ref if own else rows.at[src]
        cut = pl.ds(k * part, part)
        return pltpu.make_async_remote_copy(
            src_ref=here.at[cut], dst_ref=rows.at[src, cut],
            send_sem=send.at[src, k], recv_sem=r_r.at[src, k],
            device_id=(b, there), device_id_type=MESH)

    def up(src, k, own=False):
        return hop(src, k, v + 2, up_s, own)

    def down(src, k, own=False):
        return hop(src, k, v - 2, dn_s, own)

    def place(i, q):
        return i // SUB, pl.ds(pl.multiple_of(q * quarter + (i % SUB) * piece, piece), piece)

    def w_y(i):
        t, cut = place(i, b)
        cols = pl.ds(pl.multiple_of(t * TILE, TILE), TILE)
        return pltpu.make_async_remote_copy(
            src_ref=w_ref.at[cut, cols], dst_ref=wv.at[tiles + t, cut],
            send_sem=y_s.at[i], recv_sem=y_r.at[i], device_id=(b, yp), device_id_type=MESH)

    def relay(i, q, send, recv, to):
        t, cut = place(i, q)
        there = wv.at[tiles + t, cut]
        return pltpu.make_async_remote_copy(
            src_ref=there, dst_ref=there, send_sem=send, recv_sem=recv,
            device_id=(to, v), device_id_type=MESH)

    def w_x(i, q):
        return relay(i, q, x_s.at[i], x_r.at[i], xb)

    def w_d(i, q, k):
        return relay(i, q, d_s.at[k, i], d_r.at[k, i], cb)

    for k in range(CHUNKS):
        @pl.when(z < n - 1)
        def _():
            up(z, k, True).start()

        @pl.when(z > 0)
        def _():
            down(z, k, True).start()

    @pl.loop(0, total)
    def _(i):
        w_y(i).start()

    own_rows.wait()
    for t in range(tiles):
        own_w(t).wait()

    def order(o):
        low = z < 2
        zz = jnp.where(low, z, n - 1 - z)
        s = jnp.where(o == 0, zz, jnp.where(o == 1, 1 - zz, o))
        return jnp.where(low, s, n - 1 - s)

    def row_event(d, k):
        below, above = z - d, z + d

        @pl.when(below >= 0)
        def _():
            up(below, k).wait_recv()

            @pl.when(z < n - 1)
            def _():
                up(below, k).start()

        @pl.when(above < n)
        def _():
            down(above, k).wait_recv()

            @pl.when(z > 0)
            def _():
                down(above, k).start()

    def product(src, t):
        lg[src, t] = jnp.dot(rows[src], wv[t], preferred_element_type=jnp.float32)

    def trees():
        r_id = lax.broadcasted_iota(jnp.int32, (LANES, LANES), 0)
        n_id = lax.broadcasted_iota(jnp.int32, (LANES, LANES), 1)
        for p in range(pairs):
            up_of = par_ref[pl.ds(p, 1), :] == r_id
            pick[p] = up_of.astype(jnp.float32).astype(jnp.bfloat16)
            jump[p] = (up_of & (n_id % nodes != 0)).astype(jnp.float32).astype(jnp.bfloat16)
            anc[p] = (r_id == n_id).astype(jnp.float32).astype(jnp.bfloat16)

        @pl.loop(0, (nodes - 1).bit_length())
        def _(k):
            for p in range(pairs):
                a, j = anc[p], jump[p]
                more = jnp.dot(a, j, preferred_element_type=jnp.float32)
                twice = jnp.dot(j, j, preferred_element_type=jnp.float32)
                anc[p] = (a.astype(jnp.float32) + more).astype(jnp.bfloat16)
                jump[p] = twice.astype(jnp.bfloat16)

    steps = plan(tiles)
    tasks, first = [], []
    last_step = max(SUB * tiles + 2, 2 * CHUNKS * (n - 1) - 2)
    for i in range(last_step + 1):
        first.append(len(tasks))
        tasks += steps.get(i, [])
    first.append(len(tasks))

    @pl.loop(0, last_step + 1)
    def _(i):
        @pl.when(i < total)
        def _():
            w_y(i).wait_recv()
            w_x(i, b).start()
            w_d(i, b, 0).start()

        @pl.when((i >= 1) & (i <= total))
        def _():
            w_x(i - 1, xb).wait_recv()
            w_d(i - 1, xb, 1).start()
            w_d(i - 1, cb, 0).wait_recv()

        @pl.when((i >= 2) & (i <= total + 1))
        def _():
            w_d(i - 2, cxb, 1).wait_recv()

        @pl.when((i % 2 == 1) & (i < 2 * CHUNKS * (n - 1) - 1))
        def _():
            j = i // 2
            row_event(j // CHUNKS + 1, j % CHUNKS)

        @pl.when(i == 7)
        def _():
            trees()

        def run(g, c):
            o = table(g, [a for a, _ in tasks])
            t = table(g, [a for _, a in tasks])
            product(order(o), t)
            return c

        lax.fori_loop(table(i, first[:-1]), table(i, first[1:]), run, 0)

    def stats(src):
        here = 2 * src + y
        draft = draft_ref[pl.ds(here, 1), :]

        def top(t, m):
            l = lg[src, t]
            for k in range(0, TILE, LANES):
                m = jnp.maximum(m, l[:, k:k + LANES])
            return m

        mx = lax.fori_loop(1, 2 * tiles, top, jnp.maximum(lg[src, 0, :, :LANES], lg[src, 0, :, LANES:2 * LANES]))
        m = jnp.max(mx, axis=1, keepdims=True)
        c_id = lax.broadcasted_iota(jnp.int32, (TILE, LANES), 0)

        def body(t, carry):
            s, g = carry
            l = lg[src, t]
            e = jnp.exp(l - m)
            for k in range(0, TILE, LANES):
                s = s + e[:, k:k + LANES]
            base = jnp.where(t < tiles, v * width + t * TILE, yp * width + (t - tiles) * TILE)
            hot = (c_id == draft - base).astype(jnp.float32).astype(jnp.bfloat16)
            for a in split3(l):
                g = g + jnp.dot(a, hot, preferred_element_type=jnp.float32)
            return s, g

        zero = jnp.zeros((count, LANES), jnp.float32)
        s, g = lax.fori_loop(0, 2 * tiles, body, (zero, zero))
        r_id = lax.broadcasted_iota(jnp.int32, (LANES, LANES), 0)
        t_row = jnp.sum(jnp.where(par_ref[pl.ds(here, 1), :] == r_id, g, 0.0), axis=0, keepdims=True)
        m_row = jnp.max(mx.T, axis=0, keepdims=True)
        s_row = jnp.sum(s.T, axis=0, keepdims=True)
        sub = lax.broadcasted_iota(jnp.int32, (8, LANES), 0)
        st[v, src] = jnp.where(sub == 0, m_row, jnp.where(sub == 1, s_row, jnp.where(sub == 2, t_row, 0.0)))

    @pl.loop(0, n)
    def _(o):
        src = order(o)

        @pl.when(o == n - 1)
        def _():
            row_event(n - 1, CHUNKS - 1)

            @pl.loop(0, 2 * tiles)
            def _(t):
                product(src, t)

        stats(src)

    def tell(k):
        return pltpu.make_async_remote_copy(
            src_ref=st.at[v], dst_ref=st.at[v], send_sem=st_s.at[k], recv_sem=st_r.at[v],
            device_id=(b, lax.rem(v + k, peers)), device_id_type=MESH)

    def heard(k):
        other = lax.rem(v + k, peers)
        return pltpu.make_async_remote_copy(
            src_ref=st.at[other], dst_ref=st.at[other], send_sem=st_s.at[k], recv_sem=st_r.at[other],
            device_id=(b, other), device_id_type=MESH)

    for k in range(1, peers):
        tell(k).start()

    @pl.loop(0, total)
    def _(i):
        w_y(i).wait_send()
        w_x(i, b).wait_send()
        w_d(i, b, 0).wait_send()
        w_d(i, xb, 1).wait_send()

    @pl.loop(0, n)
    def _(src):
        @pl.loop(0, CHUNKS)
        def _(k):
            @pl.when((src <= z) & (z < n - 1))
            def _():
                up(src, k).wait_send()

            @pl.when((src >= z) & (z > 0))
            def _():
                down(src, k).wait_send()

    for k in range(1, peers):
        heard(k).wait_recv()

    sub = lax.broadcasted_iota(jnp.int32, (16, LANES), 0)
    lane = lax.broadcasted_iota(jnp.int32, (1, LANES), 1)

    def through(row, mat):
        hi, mid, lo = [a.astype(jnp.float32) for a in split3(row)]
        lhs = jnp.where(sub == 0, hi, jnp.where(sub == 1, mid, jnp.where(sub == 2, lo, 0.0)))
        return jnp.sum(jnp.dot(lhs.astype(jnp.bfloat16), mat, preferred_element_type=jnp.float32), axis=0, keepdims=True)

    for p in range(pairs):
        src, yy = p // 2, p % 2
        got = [st[2 * k + yy, src] for k in range(n)]
        ms = [g[0:1] for g in got]
        m = functools.reduce(jnp.maximum, ms)
        s = sum(g[1:2] * jnp.exp(a - m) for g, a in zip(got, ms))
        lt = m + jnp.log(s)
        target = sum(g[2:3] for g in got)
        dl = jnp.where(lane % nodes > 0, target - through(lt, pick[p]), 0.0)
        ps = through(dl, anc[p])
        for ref, row in ((lt_ref, lt), (dl_ref, dl), (ps_ref, ps)):
            ref[pl.ds(2 * p, 1), :] = row[:, :nodes]
            ref[pl.ds(2 * p + 1, 1), :] = pltpu.roll(row, nodes, 1)[:, :nodes]

    for k in range(1, peers):
        tell(k).wait_send()


def per_device(n, hidden_rows, head_weight, draft_ids, parents):
    seqs, nodes = draft_ids.shape
    count, depth = hidden_rows.shape
    tiles = head_weight.shape[1] // TILE
    pairs = seqs // 2
    drafts = draft_ids.reshape(pairs, 2 * nodes)
    pars = (parents + nodes * (jnp.arange(seqs, dtype=jnp.int32) % 2)[:, None]).reshape(pairs, 2 * nodes)
    out = jax.ShapeDtypeStruct((seqs, nodes), jnp.float32)
    vmem = pl.BlockSpec(memory_space=pltpu.VMEM)
    hbm = pl.BlockSpec(memory_space=pl.ANY)
    dma = pltpu.SemaphoreType.DMA
    total = tiles * SUB
    return pl.pallas_call(
        functools.partial(kernel, n, nodes),
        out_shape=(out, out, out),
        in_specs=[hbm, hbm, vmem, vmem],
        out_specs=(vmem, vmem, vmem),
        scratch_shapes=[
            pltpu.VMEM((n, count, depth), jnp.bfloat16),
            pltpu.VMEM((2 * tiles, depth, TILE), jnp.bfloat16),
            pltpu.VMEM((n, 2 * tiles, count, TILE), jnp.float32),
            pltpu.VMEM((2 * n, n, 8, LANES), jnp.float32),
            pltpu.VMEM((pairs, LANES, LANES), jnp.bfloat16),
            pltpu.VMEM((pairs, LANES, LANES), jnp.bfloat16),
            pltpu.VMEM((pairs, LANES, LANES), jnp.bfloat16),
            dma((n, CHUNKS)), dma((n, CHUNKS)), dma((n, CHUNKS)),
            dma((total,)), dma((total,)), dma((total,)), dma((total,)),
            dma((2, total)), dma((2, total)),
            dma((2 * n,)), dma((2 * n,)),
            dma((tiles,)), dma,
        ],
        compiler_params=pltpu.CompilerParams(
            collective_id=0, has_side_effects=True, vmem_limit_bytes=56 * 1024 * 1024
        ),
    )(hidden_rows, head_weight, drafts, pars)


def solution(mesh):
    placed = (P(("batch", "vocab"), None), P(None, "vocab"), P("batch", None), P("batch", None))
    batch, vocab = mesh.shape["batch"], mesh.shape["vocab"]

    def choose(hidden_rows, head_weight, draft_ids, parents):
        count = hidden_rows.shape[0]
        fits = batch == 4 and vocab == 8 and count == 2 * draft_ids.shape[1] == LANES
        fits = fits and head_weight.shape[1] == 5 * TILE
        if fits:
            return per_device(vocab // 2, hidden_rows, head_weight, draft_ids, parents)
        return general(hidden_rows, head_weight, draft_ids, parents)

    return jax.shard_map(
        choose,
        mesh=mesh,
        in_specs=placed,
        out_specs=(P("batch", None), P("batch", None), P("batch", None)),
        check_vma=False,
    )
```

```python
import functools

import jax
import jax.numpy as jnp
from jax import lax
from jax.experimental import pallas as pl
from jax.experimental.pallas import tpu as pltpu
from jax.sharding import PartitionSpec as P

MESH = pl.DeviceIdType.MESH
LANES = 128
TILE = 256
SUB = 4
CHUNKS = 4


def general(hidden_rows, head_weight, draft_ids, parents):
    shard_width = head_weight.shape[1]
    offset = lax.axis_index("vocab") * shard_width
    gathered = lax.all_gather(hidden_rows, "vocab", axis=0, tiled=True)
    logits = jnp.dot(gathered, head_weight, preferred_element_type=jnp.float32)
    seq_count, node_count = draft_ids.shape
    node_ids = jnp.arange(node_count, dtype=jnp.int32)
    local_max = jnp.max(logits, axis=1)
    parent_rows = (jnp.arange(seq_count, dtype=jnp.int32)[:, None] * node_count + parents).reshape(
        -1
    )
    columns = draft_ids.reshape(-1) - offset
    inside = (columns >= 0) & (columns < shard_width)
    picked = jnp.take(
        logits.reshape(-1), parent_rows * shard_width + jnp.clip(columns, 0, shard_width - 1)
    )
    local_target = jnp.where(inside, picked, jnp.zeros_like(picked))
    row_top = lax.pmax(local_max, "vocab")
    local_sum = jnp.sum(jnp.exp(logits - row_top[:, None]), axis=1)
    row_total, target = lax.psum((local_sum, local_target), "vocab")
    log_total = (row_top + jnp.log(row_total)).reshape(seq_count, node_count)
    target = target.reshape(seq_count, node_count)
    choose = (parents[:, :, None] == node_ids[None, None, :]).astype(jnp.float32)
    log_parent = jnp.einsum("snr,sr->sn", choose, log_total, precision=lax.Precision.HIGHEST)
    draft_logp = jnp.where(node_ids[None, :] > 0, target - log_parent, jnp.zeros_like(target))
    path_sum = draft_logp
    jump_table = choose
    for jump_round in range((node_count - 1).bit_length()):
        path_sum = path_sum + jnp.einsum(
            "snr,sr->sn", jump_table, path_sum, precision=lax.Precision.HIGHEST
        )
        jump_table = jnp.einsum(
            "snr,srq->snq", jump_table, jump_table, precision=lax.Precision.HIGHEST
        )
    return (log_total, draft_logp, path_sum)


def plan(tiles):
    steps = {}
    for t in range(tiles):
        steps.setdefault(1 + t, []).append((0, t))
    for t in range(tiles):
        steps.setdefault(8 + t // 2, []).append((1, t))
        steps.setdefault(16 + t // 2, []).append((2, t))
    for j in range(tiles):
        ready = SUB * j + SUB + 1
        for o, come in ((0, 6), (1, 10), (2, 18)):
            steps.setdefault(max(ready, come), []).append((o, tiles + j))
    return steps


def table(index, values):
    out = jnp.int32(values[-1])
    for k in range(len(values) - 2, -1, -1):
        if values[k] != values[k + 1]:
            out = jnp.where(index <= k, jnp.int32(values[k]), out)
    return out


def split2(x):
    hi = x.astype(jnp.bfloat16)
    return hi, (x - hi.astype(jnp.float32)).astype(jnp.bfloat16)


def split3(x):
    hi = x.astype(jnp.bfloat16)
    rest = x - hi.astype(jnp.float32)
    mid = rest.astype(jnp.bfloat16)
    lo = (rest - mid.astype(jnp.float32)).astype(jnp.bfloat16)
    return hi, mid, lo


def kernel(n, nodes, h_ref, w_ref, ids_ref, up_ref, lt_ref, dl_ref, ps_ref,
           draft_ref, par_ref, rows, wv, lg, mxa, gac, st, pick, anc, jump,
           up_s, dn_s, r_r, y_s, y_r, x_s, x_r, d_s, d_r, st_s, st_r, loc_w, loc_r):
    b, v = lax.axis_index("batch"), lax.axis_index("vocab")
    x, z, y = b // 2, v // 2, v % 2
    peers = 2 * n
    yp = v + 1 - 2 * y
    xb = b + 2 - 4 * x
    cb = b + 1 - 2 * (b % 2)
    cxb = cb + 2 - 4 * x
    count, depth = h_ref.shape
    width = w_ref.shape[1]
    tiles = width // TILE
    quarter = depth // 4
    piece = quarter // SUB
    part = count // CHUNKS
    total = tiles * SUB
    pairs = par_ref.shape[0]

    barrier = pltpu.get_barrier_semaphore()
    for k in range(1, peers):
        pl.semaphore_signal(barrier, inc=1, device_id=(b, lax.rem(v + k, peers)), device_id_type=MESH)
    pl.semaphore_signal(barrier, inc=1, device_id=(cb, v), device_id_type=MESH)
    pl.semaphore_signal(barrier, inc=1, device_id=(xb, v), device_id_type=MESH)

    def own_w(t):
        return pltpu.make_async_copy(w_ref.at[:, pl.ds(t * TILE, TILE)], wv.at[t], loc_w.at[t])

    own_rows = pltpu.make_async_copy(h_ref, rows.at[z], loc_r)
    own_rows.start()
    for t in range(tiles):
        own_w(t).start()
    pl.semaphore_wait(barrier, peers + 1)

    def hop(src, k, there, send, own):
        here = h_ref if own else rows.at[src]
        cut = pl.ds(k * part, part)
        return pltpu.make_async_remote_copy(
            src_ref=here.at[cut], dst_ref=rows.at[src, cut],
            send_sem=send.at[src, k], recv_sem=r_r.at[src, k],
            device_id=(b, there), device_id_type=MESH)

    def up(src, k, own=False):
        return hop(src, k, v + 2, up_s, own)

    def down(src, k, own=False):
        return hop(src, k, v - 2, dn_s, own)

    def place(i, q):
        return i // SUB, pl.ds(pl.multiple_of(q * quarter + (i % SUB) * piece, piece), piece)

    def w_y(i):
        t, cut = place(i, b)
        cols = pl.ds(pl.multiple_of(t * TILE, TILE), TILE)
        return pltpu.make_async_remote_copy(
            src_ref=w_ref.at[cut, cols], dst_ref=wv.at[tiles + t, cut],
            send_sem=y_s.at[i], recv_sem=y_r.at[i], device_id=(b, yp), device_id_type=MESH)

    def relay(i, q, send, recv, to):
        t, cut = place(i, q)
        there = wv.at[tiles + t, cut]
        return pltpu.make_async_remote_copy(
            src_ref=there, dst_ref=there, send_sem=send, recv_sem=recv,
            device_id=(to, v), device_id_type=MESH)

    def w_x(i, q):
        return relay(i, q, x_s.at[i], x_r.at[i], xb)

    def w_d(i, q, k):
        return relay(i, q, d_s.at[k, i], d_r.at[k, i], cb)

    for k in range(CHUNKS):
        @pl.when(z < n - 1)
        def _():
            up(z, k, True).start()

        @pl.when(z > 0)
        def _():
            down(z, k, True).start()

    @pl.loop(0, total)
    def _(i):
        w_y(i).start()

    for p in range(pairs):
        one, two = pl.ds(2 * p, 1), pl.ds(2 * p + 1, 1)
        draft_ref[p:p + 1, :nodes] = ids_ref[one, :]
        draft_ref[p:p + 1, nodes:] = ids_ref[two, :]
        par_ref[p:p + 1, :nodes] = up_ref[one, :]
        par_ref[p:p + 1, nodes:] = up_ref[two, :] + nodes
    mxa[...] = jnp.full_like(mxa, -jnp.inf)
    gac[...] = jnp.zeros_like(gac)
    r_id = lax.broadcasted_iota(jnp.int32, (LANES, LANES), 0)
    n_id = lax.broadcasted_iota(jnp.int32, (LANES, LANES), 1)
    for p in range(pairs):
        up_of = par_ref[pl.ds(p, 1), :] == r_id
        pick[p] = up_of.astype(jnp.float32).astype(jnp.bfloat16)
        jump[p] = (up_of & (n_id % nodes != 0)).astype(jnp.float32).astype(jnp.bfloat16)
        anc[p] = (r_id == n_id).astype(jnp.float32).astype(jnp.bfloat16)

    @pl.loop(0, (nodes - 1).bit_length())
    def _(k):
        for p in range(pairs):
            a, j = anc[p], jump[p]
            more = jnp.dot(a, j, preferred_element_type=jnp.float32)
            twice = jnp.dot(j, j, preferred_element_type=jnp.float32)
            anc[p] = (a.astype(jnp.float32) + more).astype(jnp.bfloat16)
            jump[p] = twice.astype(jnp.bfloat16)

    own_rows.wait()
    for t in range(tiles):
        own_w(t).wait()

    def order(o):
        low = z < 2
        zz = jnp.where(low, z, n - 1 - z)
        s = jnp.where(o == 0, zz, jnp.where(o == 1, 1 - zz, o))
        return jnp.where(low, s, n - 1 - s)

    def row_event(d, k):
        below, above = z - d, z + d

        @pl.when(below >= 0)
        def _():
            up(below, k).wait_recv()

            @pl.when(z < n - 1)
            def _():
                up(below, k).start()

        @pl.when(above < n)
        def _():
            down(above, k).wait_recv()

            @pl.when(z > 0)
            def _():
                down(above, k).start()

    def product(src, t, low=0, size=None):
        size = size or count
        cut = pl.ds(low, size)
        l = jnp.dot(rows[src, cut, :], wv[t], preferred_element_type=jnp.float32)
        lg[src, t, cut, :] = l
        m = mxa[src, cut, :]
        for k in range(0, TILE, LANES):
            m = jnp.maximum(m, l[:, k:k + LANES])
        mxa[src, cut, :] = m
        here = 2 * src + y
        base = jnp.where(t < tiles, v * width + t * TILE, yp * width + (t - tiles) * TILE)
        c_id = lax.broadcasted_iota(jnp.int32, (TILE, LANES), 0)
        hot = (c_id == draft_ref[pl.ds(here, 1), :] - base).astype(jnp.float32).astype(jnp.bfloat16)
        both = jnp.dot(jnp.concatenate(split2(l), axis=0), hot, preferred_element_type=jnp.float32)
        gac[src, cut, :] += both[:size] + both[size:]

    steps = plan(tiles)
    tasks, first = [], []
    last_step = max(SUB * tiles + 1, 2 * (CHUNKS * (n - 1) - 2) - 1)
    for i in range(last_step + 1):
        first.append(len(tasks))
        tasks += steps.get(i, [])
    first.append(len(tasks))

    @pl.loop(0, last_step + 1)
    def _(i):
        @pl.when(i < total)
        def _():
            w_y(i).wait_recv()
            w_x(i, b).start()
            w_d(i, b, 0).start()

        @pl.when((i >= 1) & (i <= total))
        def _():
            w_x(i - 1, xb).wait_recv()
            w_d(i - 1, xb, 1).start()
            w_d(i - 1, cb, 0).wait_recv()

        @pl.when((i >= 2) & (i <= total + 1))
        def _():
            w_d(i - 2, cxb, 1).wait_recv()

        @pl.when((i % 2 == 1) & (i < 2 * (CHUNKS * (n - 1) - 2)))
        def _():
            j = i // 2
            row_event(j // CHUNKS + 1, j % CHUNKS)

        def run(g, c):
            o = table(g, [a for a, _ in tasks])
            t = table(g, [a for _, a in tasks])
            product(order(o), t)
            return c

        lax.fori_loop(table(i, first[:-1]), table(i, first[1:]), run, 0)

    def stats(src):
        here = 2 * src + y
        mx = mxa[src]
        m = jnp.max(mx, axis=1, keepdims=True)
        sums = []
        for r in range(0, count, 32):
            s = jnp.zeros((32, LANES), jnp.float32)
            for t in range(2 * tiles):
                for k in range(0, TILE, LANES):
                    s = s + jnp.exp(lg[src, t, r:r + 32, k:k + LANES] - m[r:r + 32])
            sums.append(s)
        s = jnp.concatenate(sums, axis=0)
        r_id = lax.broadcasted_iota(jnp.int32, (LANES, LANES), 0)
        t_row = jnp.sum(jnp.where(par_ref[pl.ds(here, 1), :] == r_id, gac[src], 0.0), axis=0, keepdims=True)
        m_row = jnp.max(mx.T, axis=0, keepdims=True)
        s_row = jnp.sum(s.T, axis=0, keepdims=True)
        sub = lax.broadcasted_iota(jnp.int32, (8, LANES), 0)
        st[v, src] = jnp.where(sub == 0, m_row, jnp.where(sub == 1, s_row, jnp.where(sub == 2, t_row, 0.0)))

    last = order(n - 1)
    half = count // 2

    @pl.loop(0, 2 * tiles)
    def _(t):
        product(last, t, 0, half)

    @pl.loop(0, n)
    def _(o):
        @pl.when(o == n - 1)
        def _():
            row_event(n - 1, CHUNKS - 2)
            row_event(n - 1, CHUNKS - 1)

            @pl.loop(0, 2 * tiles)
            def _(t):
                product(last, t, half, half)

        stats(order(o))

    def tell(k):
        return pltpu.make_async_remote_copy(
            src_ref=st.at[v], dst_ref=st.at[v], send_sem=st_s.at[k], recv_sem=st_r.at[v],
            device_id=(b, lax.rem(v + k, peers)), device_id_type=MESH)

    def heard(k):
        other = lax.rem(v + k, peers)
        return pltpu.make_async_remote_copy(
            src_ref=st.at[other], dst_ref=st.at[other], send_sem=st_s.at[k], recv_sem=st_r.at[other],
            device_id=(b, other), device_id_type=MESH)

    for k in range(1, peers):
        tell(k).start()

    @pl.loop(0, total)
    def _(i):
        w_y(i).wait_send()
        w_x(i, b).wait_send()
        w_d(i, b, 0).wait_send()
        w_d(i, xb, 1).wait_send()

    @pl.loop(0, n)
    def _(src):
        @pl.loop(0, CHUNKS)
        def _(k):
            @pl.when((src <= z) & (z < n - 1))
            def _():
                up(src, k).wait_send()

            @pl.when((src >= z) & (z > 0))
            def _():
                down(src, k).wait_send()

    for k in range(1, peers):
        heard(k).wait_recv()

    sub = lax.broadcasted_iota(jnp.int32, (16, LANES), 0)
    lane = lax.broadcasted_iota(jnp.int32, (1, LANES), 1)

    def through(row, mat):
        hi, mid, lo = [a.astype(jnp.float32) for a in split3(row)]
        lhs = jnp.where(sub == 0, hi, jnp.where(sub == 1, mid, jnp.where(sub == 2, lo, 0.0)))
        return jnp.sum(jnp.dot(lhs.astype(jnp.bfloat16), mat, preferred_element_type=jnp.float32), axis=0, keepdims=True)

    for p in range(pairs):
        src, yy = p // 2, p % 2
        got = [st[2 * k + yy, src] for k in range(n)]
        ms = [g[0:1] for g in got]
        m = functools.reduce(jnp.maximum, ms)
        s = sum(g[1:2] * jnp.exp(a - m) for g, a in zip(got, ms))
        lt = m + jnp.log(s)
        target = sum(g[2:3] for g in got)
        dl = jnp.where(lane % nodes > 0, target - through(lt, pick[p]), 0.0)
        ps = through(dl, anc[p])
        for ref, row in ((lt_ref, lt), (dl_ref, dl), (ps_ref, ps)):
            ref[pl.ds(2 * p, 1), :] = row[:, :nodes]
            ref[pl.ds(2 * p + 1, 1), :] = pltpu.roll(row, nodes, 1)[:, :nodes]

    for k in range(1, peers):
        tell(k).wait_send()


def hand_on(a_ref, b_ref, c_ref, x_ref, y_ref, z_ref):
    x_ref[...] = a_ref[...]
    y_ref[...] = b_ref[...]
    z_ref[...] = c_ref[...]


def per_device(n, hidden_rows, head_weight, draft_ids, parents):
    seqs, nodes = draft_ids.shape
    count, depth = hidden_rows.shape
    tiles = head_weight.shape[1] // TILE
    pairs = seqs // 2
    out = jax.ShapeDtypeStruct((seqs, nodes), jnp.float32)
    vmem = pl.BlockSpec(memory_space=pltpu.VMEM)
    hbm = pl.BlockSpec(memory_space=pl.ANY)
    dma = pltpu.SemaphoreType.DMA
    total = tiles * SUB
    found = pl.pallas_call(
        functools.partial(kernel, n, nodes),
        out_shape=(out, out, out),
        in_specs=[hbm, hbm, vmem, vmem],
        out_specs=(vmem, vmem, vmem),
        scratch_shapes=[
            pltpu.VMEM((pairs, LANES), jnp.int32),
            pltpu.VMEM((pairs, LANES), jnp.int32),
            pltpu.VMEM((n, count, depth), jnp.bfloat16),
            pltpu.VMEM((2 * tiles, depth, TILE), jnp.bfloat16),
            pltpu.VMEM((n, 2 * tiles, count, TILE), jnp.float32),
            pltpu.VMEM((n, count, LANES), jnp.float32),
            pltpu.VMEM((n, count, LANES), jnp.float32),
            pltpu.VMEM((2 * n, n, 8, LANES), jnp.float32),
            pltpu.VMEM((pairs, LANES, LANES), jnp.bfloat16),
            pltpu.VMEM((pairs, LANES, LANES), jnp.bfloat16),
            pltpu.VMEM((pairs, LANES, LANES), jnp.bfloat16),
            dma((n, CHUNKS)), dma((n, CHUNKS)), dma((n, CHUNKS)),
            dma((total,)), dma((total,)), dma((total,)), dma((total,)),
            dma((2, total)), dma((2, total)),
            dma((2 * n,)), dma((2 * n,)),
            dma((tiles,)), dma,
        ],
        compiler_params=pltpu.CompilerParams(
            collective_id=0, has_side_effects=True, vmem_limit_bytes=56 * 1024 * 1024
        ),
    )(hidden_rows, head_weight, draft_ids, parents)
    return pl.pallas_call(
        hand_on,
        out_shape=(out, out, out),
        in_specs=[vmem] * 3,
        out_specs=(vmem, vmem, vmem),
    )(*found)


def solution(mesh):
    placed = (P(("batch", "vocab"), None), P(None, "vocab"), P("batch", None), P("batch", None))
    batch, vocab = mesh.shape["batch"], mesh.shape["vocab"]

    def choose(hidden_rows, head_weight, draft_ids, parents):
        count = hidden_rows.shape[0]
        fits = batch == 4 and vocab == 8 and count == 2 * draft_ids.shape[1] == LANES
        fits = fits and head_weight.shape[1] == 5 * TILE
        if fits:
            return per_device(vocab // 2, hidden_rows, head_weight, draft_ids, parents)
        return general(hidden_rows, head_weight, draft_ids, parents)

    return jax.shard_map(
        choose,
        mesh=mesh,
        in_specs=placed,
        out_specs=(P("batch", None), P("batch", None), P("batch", None)),
        check_vma=False,
    )
```

```python
import functools

import jax
import jax.numpy as jnp
from jax import lax
from jax.experimental import pallas as pl
from jax.experimental.pallas import tpu as pltpu
from jax.sharding import PartitionSpec as P

MESH = pl.DeviceIdType.MESH
LANES = 128
TILE = 256
SUB = 4
CHUNKS = 4


def general(hidden_rows, head_weight, draft_ids, parents):
    shard_width = head_weight.shape[1]
    offset = lax.axis_index("vocab") * shard_width
    gathered = lax.all_gather(hidden_rows, "vocab", axis=0, tiled=True)
    logits = jnp.dot(gathered, head_weight, preferred_element_type=jnp.float32)
    seq_count, node_count = draft_ids.shape
    node_ids = jnp.arange(node_count, dtype=jnp.int32)
    local_max = jnp.max(logits, axis=1)
    parent_rows = (jnp.arange(seq_count, dtype=jnp.int32)[:, None] * node_count + parents).reshape(
        -1
    )
    columns = draft_ids.reshape(-1) - offset
    inside = (columns >= 0) & (columns < shard_width)
    picked = jnp.take(
        logits.reshape(-1), parent_rows * shard_width + jnp.clip(columns, 0, shard_width - 1)
    )
    local_target = jnp.where(inside, picked, jnp.zeros_like(picked))
    row_top = lax.pmax(local_max, "vocab")
    local_sum = jnp.sum(jnp.exp(logits - row_top[:, None]), axis=1)
    row_total, target = lax.psum((local_sum, local_target), "vocab")
    log_total = (row_top + jnp.log(row_total)).reshape(seq_count, node_count)
    target = target.reshape(seq_count, node_count)
    choose = (parents[:, :, None] == node_ids[None, None, :]).astype(jnp.float32)
    log_parent = jnp.einsum("snr,sr->sn", choose, log_total, precision=lax.Precision.HIGHEST)
    draft_logp = jnp.where(node_ids[None, :] > 0, target - log_parent, jnp.zeros_like(target))
    path_sum = draft_logp
    jump_table = choose
    for jump_round in range((node_count - 1).bit_length()):
        path_sum = path_sum + jnp.einsum(
            "snr,sr->sn", jump_table, path_sum, precision=lax.Precision.HIGHEST
        )
        jump_table = jnp.einsum(
            "snr,srq->snq", jump_table, jump_table, precision=lax.Precision.HIGHEST
        )
    return (log_total, draft_logp, path_sum)


def plan(tiles):
    steps = {}
    for t in range(tiles):
        steps.setdefault(1 + t, []).append((0, t))
    for t in range(tiles):
        steps.setdefault(8 + t // 2, []).append((1, t))
        steps.setdefault(16 + t // 2, []).append((2, t))
    for j in range(tiles):
        ready = SUB * j + SUB + 1
        for o, come in ((0, 6), (1, 10), (2, 18)):
            steps.setdefault(max(ready, come), []).append((o, tiles + j))
    return steps


def table(index, values):
    out = jnp.int32(values[-1])
    for k in range(len(values) - 2, -1, -1):
        if values[k] != values[k + 1]:
            out = jnp.where(index <= k, jnp.int32(values[k]), out)
    return out


def split2(x):
    hi = x.astype(jnp.bfloat16)
    return hi, (x - hi.astype(jnp.float32)).astype(jnp.bfloat16)


def split3(x):
    hi = x.astype(jnp.bfloat16)
    rest = x - hi.astype(jnp.float32)
    mid = rest.astype(jnp.bfloat16)
    lo = (rest - mid.astype(jnp.float32)).astype(jnp.bfloat16)
    return hi, mid, lo


def kernel(n, nodes, h_ref, w_ref, ids_ref, up_ref, lt_ref, dl_ref, ps_ref,
           draft_ref, par_ref, rows, wv, lg, mxa, gac, st, pick, anc, jump,
           up_s, dn_s, r_r, y_s, y_r, x_s, x_r, d_s, d_r, st_s, st_r, loc_w, loc_r):
    b, v = lax.axis_index("batch"), lax.axis_index("vocab")
    x, z, y = b // 2, v // 2, v % 2
    peers = 2 * n
    yp = v + 1 - 2 * y
    xb = b + 2 - 4 * x
    cb = b + 1 - 2 * (b % 2)
    cxb = cb + 2 - 4 * x
    count, depth = h_ref.shape
    width = w_ref.shape[1]
    tiles = width // TILE
    quarter = depth // 4
    piece = quarter // SUB
    part = count // CHUNKS
    total = tiles * SUB
    pairs = par_ref.shape[0]

    barrier = pltpu.get_barrier_semaphore()
    for k in range(1, peers):
        pl.semaphore_signal(barrier, inc=1, device_id=(b, lax.rem(v + k, peers)), device_id_type=MESH)
    pl.semaphore_signal(barrier, inc=1, device_id=(cb, v), device_id_type=MESH)
    pl.semaphore_signal(barrier, inc=1, device_id=(xb, v), device_id_type=MESH)

    def own_w(t):
        return pltpu.make_async_copy(w_ref.at[:, pl.ds(pl.multiple_of(t * TILE, TILE), TILE)], wv.at[t], loc_w.at[t])

    own_rows = pltpu.make_async_copy(h_ref, rows.at[z], loc_r)
    own_rows.start()
    for t in range(tiles):
        own_w(t).start()
    pl.semaphore_wait(barrier, peers + 1)

    def hop(src, k, there, send, own):
        here = h_ref if own else rows.at[src]
        cut = pl.ds(k * part, part)
        return pltpu.make_async_remote_copy(
            src_ref=here.at[cut], dst_ref=rows.at[src, cut],
            send_sem=send.at[src, k], recv_sem=r_r.at[src, k],
            device_id=(b, there), device_id_type=MESH)

    def up(src, k, own=False):
        return hop(src, k, v + 2, up_s, own)

    def down(src, k, own=False):
        return hop(src, k, v - 2, dn_s, own)

    def place(i, q):
        return i // SUB, pl.ds(pl.multiple_of(q * quarter + (i % SUB) * piece, piece), piece)

    def w_y(i):
        t, cut = place(i, b)
        cols = pl.ds(pl.multiple_of(t * TILE, TILE), TILE)
        return pltpu.make_async_remote_copy(
            src_ref=w_ref.at[cut, cols], dst_ref=wv.at[tiles + t, cut],
            send_sem=y_s.at[i], recv_sem=y_r.at[i], device_id=(b, yp), device_id_type=MESH)

    def relay(i, q, send, recv, to):
        t, cut = place(i, q)
        there = wv.at[tiles + t, cut]
        return pltpu.make_async_remote_copy(
            src_ref=there, dst_ref=there, send_sem=send, recv_sem=recv,
            device_id=(to, v), device_id_type=MESH)

    def w_x(i, q):
        return relay(i, q, x_s.at[i], x_r.at[i], xb)

    def w_d(i, q, k):
        return relay(i, q, d_s.at[k, i], d_r.at[k, i], cb)

    for k in range(CHUNKS):
        @pl.when(z < n - 1)
        def _():
            up(z, k, True).start()

        @pl.when(z > 0)
        def _():
            down(z, k, True).start()

    @pl.loop(0, total)
    def _(i):
        w_y(i).start()

    for p in range(pairs):
        one, two = pl.ds(2 * p, 1), pl.ds(2 * p + 1, 1)
        draft_ref[p:p + 1, :nodes] = ids_ref[one, :]
        draft_ref[p:p + 1, nodes:] = ids_ref[two, :]
        par_ref[p:p + 1, :nodes] = up_ref[one, :]
        par_ref[p:p + 1, nodes:] = up_ref[two, :] + nodes
    mxa[...] = jnp.full_like(mxa, -jnp.inf)
    gac[...] = jnp.zeros_like(gac)
    r_id = lax.broadcasted_iota(jnp.int32, (LANES, LANES), 0)
    n_id = lax.broadcasted_iota(jnp.int32, (LANES, LANES), 1)
    for p in range(pairs):
        up_of = par_ref[pl.ds(p, 1), :] == r_id
        pick[p] = up_of.astype(jnp.float32).astype(jnp.bfloat16)
        jump[p] = (up_of & (n_id % nodes != 0)).astype(jnp.float32).astype(jnp.bfloat16)
        anc[p] = (r_id == n_id).astype(jnp.float32).astype(jnp.bfloat16)

    def double():
        for p in range(pairs):
            a, j = anc[p], jump[p]
            more = jnp.dot(a, j, preferred_element_type=jnp.float32)
            twice = jnp.dot(j, j, preferred_element_type=jnp.float32)
            anc[p] = (a.astype(jnp.float32) + more).astype(jnp.bfloat16)
            jump[p] = twice.astype(jnp.bfloat16)

    own_rows.wait()

    def order(o):
        low = z < 2
        zz = jnp.where(low, z, n - 1 - z)
        s = jnp.where(o == 0, zz, jnp.where(o == 1, 1 - zz, o))
        return jnp.where(low, s, n - 1 - s)

    def row_event(d, k):
        below, above = z - d, z + d

        @pl.when(below >= 0)
        def _():
            up(below, k).wait_recv()

            @pl.when(z < n - 1)
            def _():
                up(below, k).start()

        @pl.when(above < n)
        def _():
            down(above, k).wait_recv()

            @pl.when(z > 0)
            def _():
                down(above, k).start()

    def picked(src, t, l):
        here = 2 * src + y
        base = jnp.where(t < tiles, v * width + t * TILE, yp * width + (t - tiles) * TILE)
        c_id = lax.broadcasted_iota(jnp.int32, (TILE, LANES), 0)
        hot = (c_id == draft_ref[pl.ds(here, 1), :] - base).astype(jnp.float32).astype(jnp.bfloat16)
        both = jnp.dot(jnp.concatenate(split2(l), axis=0), hot, preferred_element_type=jnp.float32)
        gac[src] += both[:count] + both[count:]

    def keep(src, t, l):
        lg[src, t] = l
        m = mxa[src]
        for k in range(0, TILE, LANES):
            m = jnp.maximum(m, l[:, k:k + LANES])
        mxa[src] = m

    def logits(src, t):
        return jnp.dot(rows[src], wv[t], preferred_element_type=jnp.float32)

    def product(src, t):
        l = logits(src, t)
        keep(src, t, l)
        picked(src, t, l)

    steps = plan(tiles)
    tasks, first = [], []
    last_step = max(SUB * tiles + 1, 2 * (CHUNKS * (n - 1) - 2) - 1)
    for i in range(last_step + 1):
        first.append(len(tasks))
        tasks += steps.get(i, [])
    first.append(len(tasks))

    @pl.loop(0, last_step + 1)
    def _(i):
        @pl.when(i < total)
        def _():
            w_y(i).wait_recv()
            w_x(i, b).start()
            w_d(i, b, 0).start()

        @pl.when((i >= 1) & (i <= total))
        def _():
            w_x(i - 1, xb).wait_recv()
            w_d(i - 1, xb, 1).start()
            w_d(i - 1, cb, 0).wait_recv()

        @pl.when((i >= 2) & (i <= total + 1))
        def _():
            w_d(i - 2, cxb, 1).wait_recv()

        @pl.when((i % 2 == 1) & (i < 2 * (CHUNKS * (n - 1) - 2)))
        def _():
            j = i // 2
            row_event(j // CHUNKS + 1, j % CHUNKS)

        @pl.when((i >= 1) & (i <= tiles))
        def _():
            own_w(i - 1).wait()

        @pl.when((i >= 2) & (i < 2 + (nodes - 1).bit_length()))
        def _():
            double()

        def run(g, c):
            o = table(g, [a for a, _ in tasks])
            t = table(g, [a for _, a in tasks])
            product(order(o), t)
            return c

        lax.fori_loop(table(i, first[:-1]), table(i, first[1:]), run, 0)

    def stats(src):
        here = 2 * src + y
        mx = mxa[src]
        m = jnp.max(mx, axis=1, keepdims=True)
        sums = []
        for r in range(0, count, 32):
            s = jnp.zeros((32, LANES), jnp.float32)
            for t in range(2 * tiles):
                for k in range(0, TILE, LANES):
                    s = s + jnp.exp(lg[src, t, r:r + 32, k:k + LANES] - m[r:r + 32])
            sums.append(s)
        s = jnp.concatenate(sums, axis=0)
        r_id = lax.broadcasted_iota(jnp.int32, (LANES, LANES), 0)
        t_row = jnp.sum(jnp.where(par_ref[pl.ds(here, 1), :] == r_id, gac[src], 0.0), axis=0, keepdims=True)
        m_row = jnp.max(mx.T, axis=0, keepdims=True)
        s_row = jnp.sum(s.T, axis=0, keepdims=True)
        sub = lax.broadcasted_iota(jnp.int32, (8, LANES), 0)
        st[v, src] = jnp.where(sub == 0, m_row, jnp.where(sub == 1, s_row, jnp.where(sub == 2, t_row, 0.0)))

    last = order(n - 1)

    @pl.loop(0, n)
    def _(o):
        @pl.when(o == n - 1)
        def _():
            row_event(n - 1, CHUNKS - 2)
            row_event(n - 1, CHUNKS - 1)

            keep(last, 0, logits(last, 0))

            @pl.loop(1, 2 * tiles)
            def _(t):
                before = lg[last, t - 1]
                l = logits(last, t)
                picked(last, t - 1, before)
                keep(last, t, l)

            picked(last, 2 * tiles - 1, lg[last, 2 * tiles - 1])

        stats(order(o))

    def tell(k):
        return pltpu.make_async_remote_copy(
            src_ref=st.at[v], dst_ref=st.at[v], send_sem=st_s.at[k], recv_sem=st_r.at[v],
            device_id=(b, lax.rem(v + k, peers)), device_id_type=MESH)

    def heard(k):
        other = lax.rem(v + k, peers)
        return pltpu.make_async_remote_copy(
            src_ref=st.at[other], dst_ref=st.at[other], send_sem=st_s.at[k], recv_sem=st_r.at[other],
            device_id=(b, other), device_id_type=MESH)

    for k in range(1, peers):
        tell(k).start()

    @pl.loop(0, total)
    def _(i):
        w_y(i).wait_send()
        w_x(i, b).wait_send()
        w_d(i, b, 0).wait_send()
        w_d(i, xb, 1).wait_send()

    @pl.loop(0, n)
    def _(src):
        @pl.loop(0, CHUNKS)
        def _(k):
            @pl.when((src <= z) & (z < n - 1))
            def _():
                up(src, k).wait_send()

            @pl.when((src >= z) & (z > 0))
            def _():
                down(src, k).wait_send()

    for k in range(1, peers):
        heard(k).wait_recv()

    sub = lax.broadcasted_iota(jnp.int32, (16, LANES), 0)
    lane = lax.broadcasted_iota(jnp.int32, (1, LANES), 1)

    def through(row, mat):
        hi, mid, lo = [a.astype(jnp.float32) for a in split3(row)]
        lhs = jnp.where(sub == 0, hi, jnp.where(sub == 1, mid, jnp.where(sub == 2, lo, 0.0)))
        return jnp.sum(jnp.dot(lhs.astype(jnp.bfloat16), mat, preferred_element_type=jnp.float32), axis=0, keepdims=True)

    for p in range(pairs):
        src, yy = p // 2, p % 2
        got = [st[2 * k + yy, src] for k in range(n)]
        ms = [g[0:1] for g in got]
        m = functools.reduce(jnp.maximum, ms)
        s = sum(g[1:2] * jnp.exp(a - m) for g, a in zip(got, ms))
        lt = m + jnp.log(s)
        target = sum(g[2:3] for g in got)
        dl = jnp.where(lane % nodes > 0, target - through(lt, pick[p]), 0.0)
        ps = through(dl, anc[p])
        for ref, row in ((lt_ref, lt), (dl_ref, dl), (ps_ref, ps)):
            ref[pl.ds(2 * p, 1), :] = row[:, :nodes]
            ref[pl.ds(2 * p + 1, 1), :] = pltpu.roll(row, nodes, 1)[:, :nodes]

    for k in range(1, peers):
        tell(k).wait_send()


def hand_on(a_ref, b_ref, c_ref, x_ref, y_ref, z_ref):
    x_ref[...] = a_ref[...]
    y_ref[...] = b_ref[...]
    z_ref[...] = c_ref[...]


def per_device(n, hidden_rows, head_weight, draft_ids, parents):
    seqs, nodes = draft_ids.shape
    count, depth = hidden_rows.shape
    tiles = head_weight.shape[1] // TILE
    pairs = seqs // 2
    out = jax.ShapeDtypeStruct((seqs, nodes), jnp.float32)
    vmem = pl.BlockSpec(memory_space=pltpu.VMEM)
    hbm = pl.BlockSpec(memory_space=pl.ANY)
    dma = pltpu.SemaphoreType.DMA
    total = tiles * SUB
    found = pl.pallas_call(
        functools.partial(kernel, n, nodes),
        out_shape=(out, out, out),
        in_specs=[hbm, hbm, vmem, vmem],
        out_specs=(vmem, vmem, vmem),
        scratch_shapes=[
            pltpu.VMEM((pairs, LANES), jnp.int32),
            pltpu.VMEM((pairs, LANES), jnp.int32),
            pltpu.VMEM((n, count, depth), jnp.bfloat16),
            pltpu.VMEM((2 * tiles, depth, TILE), jnp.bfloat16),
            pltpu.VMEM((n, 2 * tiles, count, TILE), jnp.float32),
            pltpu.VMEM((n, count, LANES), jnp.float32),
            pltpu.VMEM((n, count, LANES), jnp.float32),
            pltpu.VMEM((2 * n, n, 8, LANES), jnp.float32),
            pltpu.VMEM((pairs, LANES, LANES), jnp.bfloat16),
            pltpu.VMEM((pairs, LANES, LANES), jnp.bfloat16),
            pltpu.VMEM((pairs, LANES, LANES), jnp.bfloat16),
            dma((n, CHUNKS)), dma((n, CHUNKS)), dma((n, CHUNKS)),
            dma((total,)), dma((total,)), dma((total,)), dma((total,)),
            dma((2, total)), dma((2, total)),
            dma((2 * n,)), dma((2 * n,)),
            dma((tiles,)), dma,
        ],
        compiler_params=pltpu.CompilerParams(
            collective_id=0, has_side_effects=True, vmem_limit_bytes=56 * 1024 * 1024
        ),
    )(hidden_rows, head_weight, draft_ids, parents)
    return pl.pallas_call(
        hand_on,
        out_shape=(out, out, out),
        in_specs=[vmem] * 3,
        out_specs=(vmem, vmem, vmem),
    )(*found)


def solution(mesh):
    placed = (P(("batch", "vocab"), None), P(None, "vocab"), P("batch", None), P("batch", None))
    batch, vocab = mesh.shape["batch"], mesh.shape["vocab"]

    def choose(hidden_rows, head_weight, draft_ids, parents):
        count = hidden_rows.shape[0]
        fits = batch == 4 and vocab == 8 and count == 2 * draft_ids.shape[1] == LANES
        fits = fits and head_weight.shape[1] == 5 * TILE
        if fits:
            return per_device(vocab // 2, hidden_rows, head_weight, draft_ids, parents)
        return general(hidden_rows, head_weight, draft_ids, parents)

    return jax.shard_map(
        choose,
        mesh=mesh,
        in_specs=placed,
        out_specs=(P("batch", None), P("batch", None), P("batch", None)),
        check_vma=False,
    )
```
